32 devices in a mesh: rows: 16 (over z, y, x), tm: 2 (over core).
Axes of the slice: x: 2, y: 2, z: 4, core: 2. Of those that a mesh axis runs over, the one named last changes fastest.
Arguments:
- video: bfloat16 [8, 64, 96, 192], P('tm', 'rows'), may hold values from -6 to 6
- gains: float32 [4, 192], replicated, may hold values from 0.1 to 1.9
- kernels: bfloat16 [4, 3, 3, 3, 192, 192], replicated, may hold values from -0.078125 to 0.078125
Outputs:
- encoded: bfloat16 [8, 64, 96, 192], P('tm', 'rows')
The draws below stay inside these ranges and needn't reach their ends.
All inputs are finite; a program needn't handle non-finite values.
Results may differ from the reference program's by a relative error of at most 0.0065.
Values may be sent and summed in bfloat16 or wider, within the bound.
No kernel may reach another device: no remote copies, remote signals or barrier semaphores. Data moves between devices by JAX's collectives and lax.ppermute only.
A program may use at most 128 MiB of HBM per device.

```python
import jax
import jax.numpy as jnp
from jax import lax

C = 192
W = 96
FRAMES = 8
HEIGHT = 64


def block_scale(own_key, dims, pieces, low, top_value):
    factor_of = 1.0
    for position, parts in pieces:
        steps = jax.random.uniform(jax.random.fold_in(jax.random.fold_in(own_key, 6), position), (parts,), jnp.float32, low / len(pieces), top_value / len(pieces))
        factor_of = factor_of * jnp.repeat(jnp.exp(steps), dims[position] // parts).reshape((-1,) + (1,) * (len(dims) - 1 - position))
    return factor_of


def normal_values(rng, shape, scale, reach, pieces=(), dtype=jnp.bfloat16):
    drawn = jax.random.normal(rng, shape, jnp.float32) * scale
    if len(pieces) > 0:
        drawn = block_scale(rng, shape, pieces, -0.22, 0.18) * drawn
    return jnp.clip(drawn, min=-reach, max=reach).astype(dtype)


def setup_inputs(seed: int = 0) -> dict:
    splits = jax.random.split(jax.random.key(seed), 4)
    video = normal_values(splits[0], (FRAMES, HEIGHT, W, C), 1.0, 6.0, ((0, 2), (1, 16)))
    gains = jnp.clip(1.0 + 0.18 * jax.random.normal(splits[1], (4, C), jnp.float32), 0.1, 1.9)
    kernels = normal_values(splits[2], (4, 3, 3, 3, C, C), (27 * C) ** -0.5, 0.078125)
    return {"video": video, "gains": gains, "kernels": kernels}


def activate(field, gain):
    values = field.astype(jnp.float32)
    scaled = values * lax.rsqrt(lax.optimization_barrier(jnp.mean(values * values, axis=-1, keepdims=True)) + 1e-06) * gain.astype(jnp.float32)
    return jax.nn.silu(scaled).astype(jnp.bfloat16)

def convolve(field, kernel):
    result = lax.conv_general_dilated(field.astype(jnp.float32)[None], kernel.astype(jnp.float32), (1, 1, 1), [(2, 0), (1, 1), (1, 1)], dimension_numbers=('NDHWC', 'DHWIO', 'NDHWC'), precision=lax.Precision.HIGHEST)
    return result[0]

def reference(video, gains, kernels):
    hidden = video
    for block in range(2):
        first = activate(hidden, gains[2 * block])
        second = activate(convolve(first, kernels[2 * block]), gains[2 * block + 1])
        branch = convolve(second, kernels[2 * block + 1])
        hidden = (hidden.astype(jnp.float32) + branch).astype(jnp.bfloat16)
    return hidden
```

```python
import functools

import jax
import jax.numpy as jnp
from jax import lax
from jax.experimental import pallas as pl
from jax.experimental.pallas import tpu as pltpu
from jax.sharding import PartitionSpec as P

AXES = ("rows", "tm")
EPS = 1e-06
LANES = 128


def activate(x, gain):
    scale = lax.rsqrt(jnp.sum(x * x, axis=-1, keepdims=True) / x.shape[-1] + EPS)
    y = x * scale * gain
    return y / (1.0 + jnp.exp(-y))


class Shape:
    def __init__(self, width, frames, channels):
        self.width, self.frames, self.channels = width, frames, channels
        self.tile = 2 * frames
        self.size = width * frames
        self.rest = channels - LANES
        self.payload = self.size + self.size // 2
        self.chunk = next(m for m in (256, 128, 64, 32, 16) if self.size % m == 0)


def unpack(ref, start, m, sh):
    half = sh.size // 2
    a = ref[start : start + m, :]
    low = start < half
    b = ref[sh.size + start - (0 if low else half) : sh.size + start - (0 if low else half) + m, :]
    b = b[:, : sh.rest] if low else b[:, sh.rest :]
    return a.astype(jnp.float32), b.astype(jnp.float32)


def build(ref, prev, s_ref, c_ref, sh):
    m = sh.tile * 8
    f, tile, n = sh.frames, sh.tile, sh.size
    edges = []
    for start in range(0, n, m):
        parts = []
        for j, x in enumerate(unpack(ref, start, m, sh)):
            x3 = x.reshape(m // f, f, x.shape[-1])
            t = lax.broadcasted_iota(jnp.int32, x3.shape, 1)
            if prev is None:
                p3 = None
            else:
                p3 = unpack(prev, start, m, sh)[j].reshape(x3.shape)
            shifted = [x]
            for step in (1, 2):
                past = jnp.zeros_like(x3) if p3 is None else pltpu.roll(p3, step, 1)
                shifted.append(jnp.where(t >= step, pltpu.roll(x3, step, 1), past).reshape(x.shape))
            parts.append(shifted)
        (a2, a1, a0), (b2, b1, b0) = parts
        whole = jnp.concatenate([a0, a1, a2, jnp.concatenate([b0, b1], axis=1)], axis=1)
        o = tile + start
        s_ref[o : o + m, :] = whole.astype(s_ref.dtype)
        b2h = b2.astype(c_ref.dtype)
        c_ref[o + tile : o + tile + m, : sh.rest] = b2h
        c_ref[o : o + m, sh.rest : 2 * sh.rest] = b2h
        c_ref[o - tile : o - tile + m, 2 * sh.rest :] = b2h
        if start == 0:
            edges.append((whole[f : 2 * f], b2[f : 2 * f]))
        if start + m == n:
            edges.append((whole[m - 2 * f : m - f], b2[m - 2 * f : m - f]))
    (first_s, first_b), (last_s, last_b) = edges
    pad = lambda v: jnp.zeros_like(v)
    s_ref[0:tile, :] = jnp.concatenate([pad(last_s), last_s], axis=0).astype(s_ref.dtype)
    s_ref[tile + n : 2 * tile + n, :] = jnp.concatenate([first_s, pad(first_s)], axis=0).astype(s_ref.dtype)
    c_ref[tile : 2 * tile, : sh.rest] = jnp.concatenate([pad(last_b), last_b], axis=0).astype(c_ref.dtype)
    c_ref[n : n + tile, 2 * sh.rest :] = jnp.concatenate([first_b, pad(first_b)], axis=0).astype(c_ref.dtype)


def taps(s_ref, c_ref, w, base, sh):
    m, total = sh.chunk, None
    for dq in range(3):
        lhs = s_ref[pl.ds(pl.multiple_of(base + sh.tile * dq, sh.tile), m), :]
        k = [w(dt, dq) for dt in range(3)]
        rhs = jnp.concatenate([v[:LANES] for v in k] + [v[LANES:] for v in k[:2]], axis=0)
        part = jnp.dot(lhs, rhs, preferred_element_type=jnp.float32)
        total = part if total is None else total + part
    lhs = c_ref[pl.ds(pl.multiple_of(base + sh.tile, sh.tile), m), :]
    rhs = jnp.concatenate([w(2, dq)[LANES:] for dq in range(3)], axis=0)
    return total + jnp.dot(lhs, rhs, preferred_element_type=jnp.float32)


def finish(acc, base, refs, sh, second, last):
    m = sh.chunk
    here = pl.ds(base, m)
    if second:
        acc = (acc + refs["residual"][here, :].astype(jnp.float32)).astype(jnp.bfloat16)
        refs["hidden"][here, :] = acc
        acc = acc.astype(jnp.float32)
    if not last:
        refs["act"][here, :] = activate(acc, refs["gain"][...])


def pack(act_ref, out_ref, sh):
    n, half = sh.size, sh.size // 2
    out_ref[0:n, :] = act_ref[:, :LANES].astype(out_ref.dtype)
    out_ref[n:, :] = jnp.concatenate([act_ref[:half, LANES:], act_ref[half:, LANES:]], axis=1).astype(out_ref.dtype)


def scratch(rows, sh):
    return [pltpu.VMEM((sh.size + 2 * sh.tile, 4 * LANES), jnp.bfloat16) for _ in range(rows)] + [
        pltpu.VMEM((sh.size + 2 * sh.tile, 3 * sh.rest), jnp.bfloat16) for _ in range(rows)
    ]


def conv_call(kind, layer, core, rows, prevs, kernels, gains, residual, partial, sh):
    second, last = layer % 2 == 1, layer == kernels.shape[0] - 1
    local = kind == "local"
    n, ch = sh.size, sh.channels
    full = lambda x: pl.BlockSpec(x.shape, lambda i, c: (0,) * x.ndim)
    ins, specs, names = [], [], []

    def add(name, value, spec=None):
        ins.append(value)
        specs.append(full(value) if spec is None else spec)
        names.append(name)

    for j, row in enumerate(rows):
        add(f"row{j}", row)
    if prevs is not None:
        for j, row in enumerate(prevs):
            add(f"prev{j}", row)
    if local:
        add("w", kernels, pl.BlockSpec((1, 3, 3, 3, ch, ch), lambda i, c: (layer, 0, 0, 0, 0, 0)))
    else:
        add("w", kernels, pl.BlockSpec((1, 3, 1, 3, ch, ch), lambda i, c: (layer, 0, 2 * c[0], 0, 0, 0)))
        add("partial", partial)
    if not last:
        add("gain", gains[layer + 1][None, :])
    if second:
        add("residual", residual)
    outs, out_names = [], []
    if local:
        outs.append(jax.ShapeDtypeStruct((n, ch), jnp.float32))
        out_names.append("rest")
    if second:
        outs.append(jax.ShapeDtypeStruct((n, ch), jnp.bfloat16))
        out_names.append("hidden")
    if not last:
        outs.append(jax.ShapeDtypeStruct((sh.payload, LANES), jnp.bfloat16))
        out_names.append("packed")
    scratches = scratch(len(rows), sh) + [pltpu.VMEM((n, ch), jnp.float32)]

    def kernel(core_ref, *refs):
        named = dict(zip(names + out_names, refs))
        s = refs[len(names) + len(out_names) :]
        k = len(rows)
        for j in range(k):
            build(named[f"row{j}"], named.get(f"prev{j}"), s[j], s[k + j], sh)
        named["act"] = s[2 * k]
        c = core_ref[0]

        def weight(dr):
            if not local:
                return lambda dt, dq: named["w"][0, dt, 0, dq]
            index = jnp.where(c == 0, dr, 2 - dr)
            return lambda dt, dq: named["w"][0, dt, index, dq]

        def step(i, carry):
            base = pl.multiple_of(i * sh.chunk, sh.chunk)
            tap = lambda row, dr: taps(s[row], s[k + row], weight(dr), base, sh)
            if local:
                inner = tap(0, 0) + tap(1, 1) + tap(2, 2)
                finish(inner, base, named, sh, second, last)
                named["rest"][pl.ds(base, sh.chunk), :] = tap(0, 1) + tap(1, 2)
            else:
                finish(named["partial"][pl.ds(base, sh.chunk), :] + tap(0, 0), base, named, sh, second, last)
            return carry

        lax.fori_loop(0, n // sh.chunk, step, 0)
        if not last:
            pack(named["act"], named["packed"], sh)

    flops = 2 * n * 9 * ch * ch * (5 if local else 1)
    got = pl.pallas_call(
        kernel,
        grid_spec=pltpu.PrefetchScalarGridSpec(
            num_scalar_prefetch=1,
            grid=(1,),
            in_specs=specs,
            out_specs=[full(o) for o in outs],
            scratch_shapes=scratches,
        ),
        out_shape=outs,
        name=f"{kind}{layer}",
        cost_estimate=pl.CostEstimate(flops=flops, transcendentals=0, bytes_accessed=4 << 20),
        compiler_params=pltpu.CompilerParams(vmem_limit_bytes=40 << 20),
    )(core, *ins)
    return dict(zip(out_names, got))


def first_call(rows, gain, sh):
    count = len(rows)
    full = lambda x: pl.BlockSpec(x.shape, lambda i: (0,) * x.ndim)

    def kernel(*refs):
        gain_ref, act = refs[count], refs[2 * count + 1]
        for j in range(count):
            def step(i, carry):
                here = pl.ds(pl.multiple_of(i * sh.chunk, sh.chunk), sh.chunk)
                act[here, :] = activate(refs[j][here, :].astype(jnp.float32), gain_ref[...])
                return carry

            lax.fori_loop(0, sh.size // sh.chunk, step, 0)
            pack(act, refs[count + 1 + j], sh)

    outs = [jax.ShapeDtypeStruct((sh.payload, LANES), jnp.bfloat16) for _ in rows]
    return pl.pallas_call(
        kernel,
        grid=(1,),
        in_specs=[full(r) for r in rows] + [full(gain)],
        out_specs=[full(o) for o in outs],
        out_shape=outs,
        scratch_shapes=[pltpu.VMEM((sh.size, sh.channels), jnp.float32)],
        name="first",
    )(*rows, gain)


def body(video, gains, kernels, count, times):
    f, height, width, ch = video.shape
    half = height // 2
    frames = 2 * f
    sh = Shape(width, frames, ch)
    device = lambda r, t: r * times + t
    index = lax.axis_index("tm")
    core = index % 2
    lower = core == 1
    chip = [(device(r, t), device(r, t ^ 1)) for r in range(count) for t in range(times)]
    outer = [(device(r, t), device(r + 1, t - 1)) for r in range(count - 1) for t in range(1, times, 2)]
    outer += [(b, a) for a, b in outer]
    later = [(device(r, t), device(r, t + 2)) for r in range(count) for t in range(times - 2)]

    top, bottom = video[:, :half], video[:, half:][:, ::-1]
    mine = jnp.where(lower, bottom, top)
    theirs = lax.ppermute(jnp.where(lower, top, bottom), AXES, chip)
    early, late = jnp.where(lower, theirs, mine), jnp.where(lower, mine, theirs)
    whole = jnp.concatenate([early, late], axis=0).reshape(frames, half, 2, width // 2, ch)
    hidden = whole.transpose(1, 3, 2, 0, 4).reshape(half, sh.size, ch)
    hidden = [hidden[j] for j in range(half)]

    packed = first_call(hidden, gains[0][None, :], sh)
    scalar = core.astype(jnp.int32)[None]
    before = (lambda rows: [lax.ppermute(row, AXES, later) for row in rows]) if times > 2 else (lambda rows: None)
    for layer in range(kernels.shape[0]):
        far = lax.ppermute(packed[0], AXES, outer)
        near = lax.ppermute(packed[-1], AXES, chip)
        rows = [packed[0], packed[1], near]
        got = conv_call("local", layer, scalar, rows, before(rows), kernels, gains, hidden[1], None, sh)
        rows = [far]
        done = conv_call("outer", layer, scalar, rows, before(rows), kernels, gains, hidden[0], got["rest"], sh)
        if "hidden" in got:
            hidden = [done["hidden"], got["hidden"]]
        if "packed" in got:
            packed = [done["packed"], got["packed"]]

    result = jnp.stack(hidden).reshape(half, width // 2, 2, frames, ch).transpose(3, 0, 2, 1, 4)
    result = result.reshape(frames, half, width, ch)
    keep = jnp.where(lower, result[f:], result[:f])
    give = jnp.where(lower, result[:f], result[f:])
    taken = lax.ppermute(give, AXES, chip)
    top, bottom = jnp.where(lower, taken, keep), jnp.where(lower, keep, taken)
    return jnp.concatenate([top, bottom[:, ::-1]], axis=1)


def solution(mesh):
    inner = functools.partial(body, count=mesh.shape["rows"], times=mesh.shape["tm"])
    specs = P("tm", "rows", None, None)
    return jax.shard_map(inner, mesh=mesh, in_specs=(specs, P(), P()), out_specs=specs, check_vma=False)
```

```python
import functools

import jax
import jax.numpy as jnp
from jax import lax
from jax.experimental import pallas as pl
from jax.experimental.pallas import tpu as pltpu
from jax.sharding import PartitionSpec as P

AXES = ("rows", "tm")
EPS = 1e-06
LANES = 128


def activate(x, gain):
    scale = lax.rsqrt(jnp.sum(x * x, axis=-1, keepdims=True) / x.shape[-1] + EPS)
    y = x * scale * (0.5 * gain)
    return y + y * jnp.tanh(y)


class Shape:
    def __init__(self, width, frames, channels):
        self.width, self.frames, self.channels = width, frames, channels
        self.tile = 2 * frames
        self.size = width * frames
        self.rest = channels - LANES
        self.payload = self.size + self.size // 2
        self.chunk = next(m for m in (256, 128, 64, 32, 16) if self.size % m == 0)


def unpack(ref, start, m, sh):
    half = sh.size // 2
    a = ref[start : start + m, :]
    low = start < half
    b = ref[sh.size + start - (0 if low else half) : sh.size + start - (0 if low else half) + m, :]
    b = b[:, : sh.rest] if low else b[:, sh.rest :]
    return a.astype(jnp.float32), b.astype(jnp.float32)


def build(ref, prev, s_ref, c_ref, sh):
    m = sh.tile * 8
    f, tile, n = sh.frames, sh.tile, sh.size
    edges = []
    for start in range(0, n, m):
        parts = []
        for j, x in enumerate(unpack(ref, start, m, sh)):
            x3 = x.reshape(m // f, f, x.shape[-1])
            t = lax.broadcasted_iota(jnp.int32, x3.shape, 1)
            if prev is None:
                p3 = None
            else:
                p3 = unpack(prev, start, m, sh)[j].reshape(x3.shape)
            shifted = [x]
            for step in (1, 2):
                past = jnp.zeros_like(x3) if p3 is None else pltpu.roll(p3, step, 1)
                shifted.append(jnp.where(t >= step, pltpu.roll(x3, step, 1), past).reshape(x.shape))
            parts.append(shifted)
        (a2, a1, a0), (b2, b1, b0) = parts
        whole = jnp.concatenate([a0, a1, a2, jnp.concatenate([b0, b1], axis=1)], axis=1)
        o = tile + start
        s_ref[o : o + m, :] = whole.astype(s_ref.dtype)
        b2h = b2.astype(c_ref.dtype)
        c_ref[o + tile : o + tile + m, : sh.rest] = b2h
        c_ref[o : o + m, sh.rest : 2 * sh.rest] = b2h
        c_ref[o - tile : o - tile + m, 2 * sh.rest :] = b2h
        if start == 0:
            edges.append((whole[f : 2 * f], b2[f : 2 * f]))
        if start + m == n:
            edges.append((whole[m - 2 * f : m - f], b2[m - 2 * f : m - f]))
    (first_s, first_b), (last_s, last_b) = edges
    pad = lambda v: jnp.zeros_like(v)
    s_ref[0:tile, :] = jnp.concatenate([pad(last_s), last_s], axis=0).astype(s_ref.dtype)
    s_ref[tile + n : 2 * tile + n, :] = jnp.concatenate([first_s, pad(first_s)], axis=0).astype(s_ref.dtype)
    c_ref[tile : 2 * tile, : sh.rest] = jnp.concatenate([pad(last_b), last_b], axis=0).astype(c_ref.dtype)
    c_ref[n : n + tile, 2 * sh.rest :] = jnp.concatenate([first_b, pad(first_b)], axis=0).astype(c_ref.dtype)


def taps(s_ref, c_ref, w, base, sh):
    m, total = sh.chunk, None
    for dq in range(3):
        lhs = s_ref[base + sh.tile * dq : base + sh.tile * dq + m, :]
        k = [w(dt, dq) for dt in range(3)]
        rhs = jnp.concatenate([v[:LANES] for v in k] + [v[LANES:] for v in k[:2]], axis=0)
        part = jnp.dot(lhs, rhs, preferred_element_type=jnp.float32)
        total = part if total is None else total + part
    lhs = c_ref[base + sh.tile : base + sh.tile + m, :]
    rhs = jnp.concatenate([w(2, dq)[LANES:] for dq in range(3)], axis=0)
    return total + jnp.dot(lhs, rhs, preferred_element_type=jnp.float32)


def finish(acc, base, refs, sh, second, last):
    m = sh.chunk
    here = slice(base, base + m)
    if second:
        acc = (acc + refs["residual"][here, :].astype(jnp.float32)).astype(jnp.bfloat16)
        if last:
            refs["act"][here, :] = acc.astype(jnp.float32)
            return
        refs["hidden"][here, :] = acc
        acc = acc.astype(jnp.float32)
    refs["act"][here, :] = activate(acc, refs["gain"][...])


def pack(act_ref, out_ref, sh):
    n, half = sh.size, sh.size // 2
    out_ref[0:n, :] = act_ref[:, :LANES].astype(out_ref.dtype)
    out_ref[n:, :] = jnp.concatenate([act_ref[:half, LANES:], act_ref[half:, LANES:]], axis=1).astype(out_ref.dtype)


def unpack_row(act_ref, keep_ref, give_ref, core, sh):
    f, w, ch = sh.frames, sh.width // 2, sh.channels
    step = 16
    for q in range(0, w, step):
        x = act_ref[q * sh.tile : (q + step) * sh.tile, :].reshape(step, 2, f, ch)
        for g in range(2):
            y = jnp.swapaxes(x[:, g], 0, 1)
            low, high = y[: f // 2], y[f // 2 :]
            here = slice(g * w + q, g * w + q + step)
            keep_ref[:, here, :] = jnp.where(core == 0, low, high).astype(keep_ref.dtype)
            give_ref[:, here, :] = jnp.where(core == 0, high, low).astype(give_ref.dtype)


def scratch(rows, sh):
    return [pltpu.VMEM((sh.size + 2 * sh.tile, 4 * LANES), jnp.bfloat16) for _ in range(rows)] + [
        pltpu.VMEM((sh.size + 2 * sh.tile, 3 * sh.rest), jnp.bfloat16) for _ in range(rows)
    ]


def conv_call(kind, layer, core, rows, prevs, weights, kernels, gains, residual, partial, sh):
    second, last = layer % 2 == 1, layer == kernels.shape[0] - 1
    local = kind == "local"
    fetch = local and not last
    n, ch = sh.size, sh.channels
    full = lambda x: pl.BlockSpec(x.shape, lambda i, c: (0,) * x.ndim)
    ins, specs, names = [], [], []

    def add(name, value, spec=None):
        ins.append(value)
        specs.append(full(value) if spec is None else spec)
        names.append(name)

    for j, row in enumerate(rows):
        add(f"row{j}", row)
    if prevs is not None:
        for j, row in enumerate(prevs):
            add(f"prev{j}", row)
    add("w", weights)
    if not local:
        add("partial", partial)
    if not last:
        add("gain", gains[layer + 1][None, :])
    if second:
        add("residual", residual)
    if fetch:
        add("kernels", kernels, pl.BlockSpec(memory_space=pltpu.HBM))
    outs, out_names = [], []

    def give(name, shape, dtype=jnp.bfloat16):
        outs.append(jax.ShapeDtypeStruct(shape, dtype))
        out_names.append(name)

    if local:
        give("rest", (n, ch), jnp.float32)
    if last:
        give("keep", (sh.frames // 2, sh.width, ch))
        give("give", (sh.frames // 2, sh.width, ch))
    else:
        if second:
            give("hidden", (n, ch))
        give("packed", (sh.payload, LANES))
    if fetch:
        give("weights", kernels.shape[1:])
    scratches = scratch(len(rows), sh) + [pltpu.VMEM((n, ch), jnp.float32), pltpu.SemaphoreType.DMA(())]

    def kernel(core_ref, *refs):
        named = dict(zip(names + out_names, refs))
        s = refs[len(names) + len(out_names) :]
        k = len(rows)
        if fetch:
            copy = pltpu.make_async_copy(named["kernels"].at[layer + 1], named["weights"], s[2 * k + 1])
            copy.start()
        for j in range(k):
            build(named[f"row{j}"], named.get(f"prev{j}"), s[j], s[k + j], sh)
        named["act"] = s[2 * k]
        c = core_ref[0]

        def weight(dr):
            index = jnp.where(c == 0, dr, 2 - dr)
            return lambda dt, dq: named["w"][dt, index, dq]

        for base in range(0, n, sh.chunk):
            tap = lambda row, dr: taps(s[row], s[k + row], weight(dr), base, sh)
            if local:
                inner = tap(0, 0) + tap(1, 1) + tap(2, 2)
                finish(inner, base, named, sh, second, last)
                named["rest"][base : base + sh.chunk, :] = tap(0, 1) + tap(1, 2)
            else:
                finish(named["partial"][base : base + sh.chunk, :] + tap(0, 0), base, named, sh, second, last)
        if last:
            unpack_row(named["act"], named["keep"], named["give"], c, sh)
        else:
            pack(named["act"], named["packed"], sh)
        if fetch:
            copy.wait()

    flops = 2 * n * 9 * ch * ch * (5 if local else 1)
    got = pl.pallas_call(
        kernel,
        grid_spec=pltpu.PrefetchScalarGridSpec(
            num_scalar_prefetch=1,
            grid=(1,),
            in_specs=specs,
            out_specs=[full(o) for o in outs],
            scratch_shapes=scratches,
        ),
        out_shape=outs,
        name=f"{kind}{layer}",
        cost_estimate=pl.CostEstimate(flops=flops, transcendentals=0, bytes_accessed=4 << 20),
        compiler_params=pltpu.CompilerParams(vmem_limit_bytes=40 << 20),
    )(core, *ins)
    return dict(zip(out_names, got))


def first_call(u, core, video, theirs, gain, kernels, sh):
    f, height, width, ch = video.shape
    half, fetch = height // 2, kernels is not None
    own_row = lambda i, c: (0, jnp.where(c[0] == 0, u, height - 1 - u), 0, 0)
    their_row = lambda i, c: (0, jnp.where(c[0] == 0, u, half - 1 - u), 0, 0)
    block = (f, 1, width, ch)
    outs = [
        jax.ShapeDtypeStruct((sh.size, ch), jnp.bfloat16),
        jax.ShapeDtypeStruct((sh.payload, LANES), jnp.bfloat16),
    ] + ([jax.ShapeDtypeStruct(kernels.shape[1:], kernels.dtype)] if fetch else [])
    full = lambda x: pl.BlockSpec(x.shape, lambda i, c: (0,) * x.ndim)

    def kernel(core_ref, own, other, gain_ref, *refs):
        if fetch:
            copy = pltpu.make_async_copy(refs[0].at[0], refs[3], refs[5])
            copy.start()
            refs = refs[1:]
        hidden, packed, act = refs[0], refs[1], refs[-2]
        c, w, step = core_ref[0], width // 2, 16
        for q in range(0, w, step):
            groups = []
            for g in range(2):
                here = slice(g * w + q, g * w + q + step)
                a, b = own[:, 0, here, :].astype(jnp.float32), other[:, 0, here, :].astype(jnp.float32)
                x = jnp.concatenate([jnp.where(c == 0, a, b), jnp.where(c == 0, b, a)], axis=0)
                groups.append(jnp.swapaxes(x, 0, 1)[:, None])
            x = jnp.concatenate(groups, axis=1).reshape(step * sh.tile, ch)
            rows = slice(q * sh.tile, (q + step) * sh.tile)
            hidden[rows, :] = x.astype(hidden.dtype)
            act[rows, :] = activate(x, gain_ref[...])
        pack(act, packed, sh)
        if fetch:
            copy.wait()

    got = pl.pallas_call(
        kernel,
        grid_spec=pltpu.PrefetchScalarGridSpec(
            num_scalar_prefetch=1,
            grid=(1,),
            in_specs=[pl.BlockSpec(block, own_row), pl.BlockSpec(block, their_row), full(gain)]
            + ([pl.BlockSpec(memory_space=pltpu.HBM)] if fetch else []),
            out_specs=[full(o) for o in outs],
            scratch_shapes=[pltpu.VMEM((sh.size, ch), jnp.float32), pltpu.SemaphoreType.DMA(())],
        ),
        out_shape=outs,
        name=f"first{u}",
        compiler_params=pltpu.CompilerParams(vmem_limit_bytes=40 << 20),
    )(core, video, theirs, gain, *([kernels] if fetch else []))
    return got


def last_call(core, keeps, takens, video, sh):
    height = video.shape[1]
    count = len(keeps)
    full = lambda x: pl.BlockSpec(x.shape, lambda i, c: (0,) * x.ndim)

    def kernel(core_ref, *refs):
        out, sems = refs[2 * count], refs[2 * count + 1]
        c = core_ref[0]
        copies = []
        for j in range(count):
            for part, upper in ((0, c == 0), (count, c != 0)):
                row = jnp.where(upper, j, height - 1 - j)
                copies.append(pltpu.make_async_copy(refs[part + j], out.at[:, row], sems.at[len(copies)]))
                copies[-1].start()
        for copy in copies:
            copy.wait()

    return pl.pallas_call(
        kernel,
        grid_spec=pltpu.PrefetchScalarGridSpec(
            num_scalar_prefetch=1,
            grid=(1,),
            in_specs=[full(k) for k in keeps + takens],
            out_specs=pl.BlockSpec(memory_space=pltpu.HBM),
            scratch_shapes=[pltpu.SemaphoreType.DMA((2 * count,))],
        ),
        out_shape=jax.ShapeDtypeStruct(video.shape, video.dtype),
        name="last",
    )(core, *keeps, *takens)


def body(video, gains, kernels, count, times):
    f, height, width, ch = video.shape
    half = height // 2
    sh = Shape(width, 2 * f, ch)
    device = lambda r, t: r * times + t
    core = lax.axis_index("tm") % 2
    scalar = core.astype(jnp.int32)[None]
    chip = [(device(r, t), device(r, t ^ 1)) for r in range(count) for t in range(times)]
    outer = [(device(r, t), device(r + 1, t - 1)) for r in range(count - 1) for t in range(1, times, 2)]
    outer += [(b, a) for a, b in outer]
    later = [(device(r, t), device(r, t + 2)) for r in range(count) for t in range(times - 2)]
    before = (lambda rows: [lax.ppermute(row, AXES, later) for row in rows]) if times > 2 else (lambda rows: None)

    give = lax.dynamic_slice_in_dim(video, (1 - core) * half, half, axis=1)
    theirs = lax.ppermute(give, AXES, chip)
    h0, p0, weights = first_call(0, scalar, video, theirs, gains[0][None, :], kernels, sh)
    h1, p1 = first_call(1, scalar, video, theirs, gains[0][None, :], None, sh)
    hidden, packed = [h0, h1], [p0, p1]
    for layer in range(kernels.shape[0]):
        far = lax.ppermute(packed[0], AXES, outer)
        near = lax.ppermute(packed[1], AXES, chip)
        rows = [packed[0], packed[1], near]
        got = conv_call("local", layer, scalar, rows, before(rows), weights, kernels, gains, hidden[1], None, sh)
        rows = [far]
        done = conv_call("outer", layer, scalar, rows, before(rows), weights, kernels, gains, hidden[0], got["rest"], sh)
        if "hidden" in got:
            hidden = [done["hidden"], got["hidden"]]
        if "packed" in got:
            packed, weights = [done["packed"], got["packed"]], got["weights"]

    takens = [lax.ppermute(part["give"], AXES, chip) for part in (done, got)]
    return last_call(scalar, [done["keep"], got["keep"]], takens, video, sh)


def solution(mesh):
    inner = functools.partial(body, count=mesh.shape["rows"], times=mesh.shape["tm"])
    specs = P("tm", "rows", None, None)
    return jax.shard_map(inner, mesh=mesh, in_specs=(specs, P(), P()), out_specs=specs, check_vma=False)
```

```python
import functools

import jax
import jax.numpy as jnp
from jax import lax
from jax.experimental import pallas as pl
from jax.experimental.pallas import tpu as pltpu
from jax.sharding import PartitionSpec as P

AXES = ("rows", "tm")
EPS = 1e-06
LANES = 128


def activate(x, gain):
    scale = lax.rsqrt(jnp.sum(x * x, axis=-1, keepdims=True) / x.shape[-1] + EPS)
    y = x * scale * (0.5 * gain)
    return y + y * jnp.tanh(y)


class Shape:
    def __init__(self, width, frames, channels):
        self.width, self.frames, self.channels = width, frames, channels
        self.tile = 2 * frames
        self.size = width * frames
        self.rest = channels - LANES
        self.payload = self.size + self.size // 2
        self.chunk = next(m for m in (256, 128, 64, 32, 16) if self.size % m == 0)


def unpack(ref, start, m, sh):
    half = sh.size // 2
    a = ref[start : start + m, :]
    low = start < half
    b = ref[sh.size + start - (0 if low else half) : sh.size + start - (0 if low else half) + m, :]
    b = b[:, : sh.rest] if low else b[:, sh.rest :]
    return a.astype(jnp.float32), b.astype(jnp.float32)


def build(ref, prev, s_ref, c_ref, sh):
    m = sh.tile * 8
    f, tile, n = sh.frames, sh.tile, sh.size
    edges = []
    for start in range(0, n, m):
        parts = []
        for j, x in enumerate(unpack(ref, start, m, sh)):
            x3 = x.reshape(m // f, f, x.shape[-1])
            t = lax.broadcasted_iota(jnp.int32, x3.shape, 1)
            if prev is None:
                p3 = None
            else:
                p3 = unpack(prev, start, m, sh)[j].reshape(x3.shape)
            shifted = [x]
            for step in (1, 2):
                past = jnp.zeros_like(x3) if p3 is None else pltpu.roll(p3, step, 1)
                shifted.append(jnp.where(t >= step, pltpu.roll(x3, step, 1), past).reshape(x.shape))
            parts.append(shifted)
        (a2, a1, a0), (b2, b1, b0) = parts
        whole = jnp.concatenate([a0, a1, a2, jnp.concatenate([b0, b1], axis=1)], axis=1)
        o = tile + start
        s_ref[o : o + m, :] = whole.astype(s_ref.dtype)
        b2h = b2.astype(c_ref.dtype)
        c_ref[o + tile : o + tile + m, : sh.rest] = b2h
        c_ref[o : o + m, sh.rest : 2 * sh.rest] = b2h
        c_ref[o - tile : o - tile + m, 2 * sh.rest :] = b2h
        if start == 0:
            edges.append((whole[f : 2 * f], b2[f : 2 * f]))
        if start + m == n:
            edges.append((whole[m - 2 * f : m - f], b2[m - 2 * f : m - f]))
    (first_s, first_b), (last_s, last_b) = edges
    pad = lambda v: jnp.zeros_like(v)
    s_ref[0:tile, :] = jnp.concatenate([pad(last_s), last_s], axis=0).astype(s_ref.dtype)
    s_ref[tile + n : 2 * tile + n, :] = jnp.concatenate([first_s, pad(first_s)], axis=0).astype(s_ref.dtype)
    c_ref[tile : 2 * tile, : sh.rest] = jnp.concatenate([pad(last_b), last_b], axis=0).astype(c_ref.dtype)
    c_ref[n : n + tile, 2 * sh.rest :] = jnp.concatenate([first_b, pad(first_b)], axis=0).astype(c_ref.dtype)


def taps(s_ref, c_ref, w, base, sh):
    m, total = sh.chunk, None
    for dq in range(3):
        lhs = s_ref[base + sh.tile * dq : base + sh.tile * dq + m, :]
        k = [w(dt, dq) for dt in range(3)]
        rhs = jnp.concatenate([v[:LANES] for v in k] + [v[LANES:] for v in k[:2]], axis=0)
        part = jnp.dot(lhs, rhs, preferred_element_type=jnp.float32)
        total = part if total is None else total + part
    lhs = c_ref[base + sh.tile : base + sh.tile + m, :]
    rhs = jnp.concatenate([w(2, dq)[LANES:] for dq in range(3)], axis=0)
    return total + jnp.dot(lhs, rhs, preferred_element_type=jnp.float32)


def finish(acc, base, refs, sh, second, last, inside=None):
    m = sh.chunk
    here = slice(base, base + m)
    if second:
        acc = (acc + refs["residual"][here, :].astype(jnp.float32)).astype(jnp.bfloat16)
        if last:
            refs["act"][here, :] = acc.astype(jnp.float32)
            return
        refs["hidden"][here, :] = acc
        acc = acc.astype(jnp.float32)
    value = activate(acc, refs["gain"][...])
    refs["act"][here, :] = value if inside is None else value * inside


def pack(act_ref, out_ref, sh):
    n, half = sh.size, sh.size // 2
    out_ref[0:n, :] = act_ref[:, :LANES].astype(out_ref.dtype)
    out_ref[n:, :] = jnp.concatenate([act_ref[:half, LANES:], act_ref[half:, LANES:]], axis=1).astype(out_ref.dtype)


def unpack_row(act_ref, keep_ref, give_ref, core, sh):
    f, w, ch = sh.frames, sh.width // 2, sh.channels
    step = 16
    for q in range(0, w, step):
        x = act_ref[q * sh.tile : (q + step) * sh.tile, :].reshape(step, 2, f, ch)
        for g in range(2):
            y = jnp.swapaxes(x[:, g], 0, 1)
            low, high = y[: f // 2], y[f // 2 :]
            here = slice(g * w + q, g * w + q + step)
            keep_ref[:, here, :] = jnp.where(core == 0, low, high).astype(keep_ref.dtype)
            give_ref[:, here, :] = jnp.where(core == 0, high, low).astype(give_ref.dtype)


def scratch(rows, sh):
    return [pltpu.VMEM((sh.size + 2 * sh.tile, 4 * LANES), jnp.bfloat16) for _ in range(rows)] + [
        pltpu.VMEM((sh.size + 2 * sh.tile, 3 * sh.rest), jnp.bfloat16) for _ in range(rows)
    ]


def conv_call(kind, layer, core, rows, prevs, weights, kernels, gains, residual, partial, sh):
    second, last = layer % 2 == 1, layer == kernels.shape[0] - 1
    local, edge = kind == "local", kind == "edge"
    ahead = not second and not edge
    fetch = local and not last
    n, ch = sh.size, sh.channels
    full = lambda x: pl.BlockSpec(x.shape, lambda i, c: (0,) * x.ndim)
    ins, specs, names = [], [], []

    def add(name, value, spec=None):
        ins.append(value)
        specs.append(full(value) if spec is None else spec)
        names.append(name)

    for j, row in enumerate(rows):
        add(f"row{j}", row)
    if prevs is not None:
        for j, row in enumerate(prevs):
            add(f"prev{j}", row)
    start = weights is None
    if not start:
        add("w", weights)
    if not local:
        add("partial", partial[0])
        if ahead:
            add("beyond", partial[1])
    if not last:
        add("gain", gains[layer + 1][None, :])
    if second:
        add("residual", residual)
    if fetch:
        add("kernels", kernels, pl.BlockSpec(memory_space=pltpu.HBM))
    outs, out_names = [], []

    def give(name, shape, dtype=jnp.bfloat16):
        outs.append(jax.ShapeDtypeStruct(shape, dtype))
        out_names.append(name)

    if local:
        give("rest", (n, ch), jnp.float32)
    if ahead:
        give("edge", (n, ch), jnp.float32)
    if last:
        give("keep", (sh.frames // 2, sh.width, ch))
        give("give", (sh.frames // 2, sh.width, ch))
    else:
        if second:
            give("hidden", (n, ch))
        give("packed", (sh.payload, LANES))
    if fetch:
        give("weights", kernels.shape[1:])
    if start:
        give("w", kernels.shape[1:])
    scratches = scratch(len(rows), sh) + [pltpu.VMEM((n, ch), jnp.float32), pltpu.SemaphoreType.DMA((2,))]

    def kernel(core_ref, *refs):
        named = dict(zip(names + out_names, refs))
        s = refs[len(names) + len(out_names) :]
        k = len(rows)
        if start:
            begin = pltpu.make_async_copy(named["kernels"].at[layer], named["w"], s[2 * k + 1].at[1])
            begin.start()
        if fetch:
            copy = pltpu.make_async_copy(named["kernels"].at[layer + 1], named["weights"], s[2 * k + 1].at[0])
            copy.start()
        for j in range(k):
            build(named[f"row{j}"], named.get(f"prev{j}"), s[j], s[k + j], sh)
        if start:
            begin.wait()
        named["act"] = s[2 * k]
        c = core_ref[0] & 1

        def weight(dr):
            index = jnp.where(c == 0, dr, 2 - dr)
            return lambda dt, dq: named["w"][dt, index, dq]

        for base in range(0, n, sh.chunk):
            here = slice(base, base + sh.chunk)
            tap = lambda row, dr: taps(s[row], s[k + row], weight(dr), base, sh)
            if local:
                named["act"][here, :] = tap(0, 0) + tap(1, 1) + tap(2, 2)
                named["rest"][here, :] = tap(0, 1) + tap(1, 2)
                if ahead:
                    named["edge"][here, :] = tap(0, 2)
            else:
                inside = (core_ref[0] >> 1).astype(jnp.float32) if edge else None
                finish(named["partial"][here, :] + tap(0, 0), base, named, sh, second, last, inside)
                if ahead:
                    named["edge"][here, :] = named["beyond"][here, :] + tap(0, 1)
        for base in range(0, n if local else 0, sh.chunk):
            finish(named["act"][base : base + sh.chunk, :], base, named, sh, second, last)
        if last:
            unpack_row(named["act"], named["keep"], named["give"], c, sh)
        else:
            pack(named["act"], named["packed"], sh)
        if fetch:
            copy.wait()

    flops = 2 * n * 9 * ch * ch * ((5 if local else 1) + ahead)
    got = pl.pallas_call(
        kernel,
        grid_spec=pltpu.PrefetchScalarGridSpec(
            num_scalar_prefetch=1,
            grid=(1,),
            in_specs=specs,
            out_specs=[full(o) for o in outs],
            scratch_shapes=scratches,
        ),
        out_shape=outs,
        name=f"{kind}{layer}",
        cost_estimate=pl.CostEstimate(flops=flops, transcendentals=0, bytes_accessed=4 << 20),
        compiler_params=pltpu.CompilerParams(vmem_limit_bytes=40 << 20),
    )(core, *ins)
    return dict(zip(out_names, got))


def first_call(u, core, mine, theirs, gain, kernels, sh):
    f, half, width, ch = mine.shape
    fetch = kernels is not None
    row = lambda i, c: (0, jnp.where((c[0] & 1) == 0, u, half - 1 - u), 0, 0)
    block = (f, 1, width, ch)
    outs = [
        jax.ShapeDtypeStruct((sh.size, ch), jnp.bfloat16),
        jax.ShapeDtypeStruct((sh.payload, LANES), jnp.bfloat16),
    ] + ([jax.ShapeDtypeStruct(kernels.shape[1:], kernels.dtype)] if fetch else [])
    full = lambda x: pl.BlockSpec(x.shape, lambda i, c: (0,) * x.ndim)

    def kernel(core_ref, own, other, gain_ref, *refs):
        if fetch:
            copy = pltpu.make_async_copy(refs[0].at[0], refs[3], refs[5])
            copy.start()
            refs = refs[1:]
        hidden, packed, act = refs[0], refs[1], refs[-2]
        c, w, step = core_ref[0] & 1, width // 2, 16
        for q in range(0, w, step):
            groups = []
            for g in range(2):
                here = slice(g * w + q, g * w + q + step)
                a, b = own[:, 0, here, :].astype(jnp.float32), other[:, 0, here, :].astype(jnp.float32)
                x = jnp.concatenate([jnp.where(c == 0, a, b), jnp.where(c == 0, b, a)], axis=0)
                groups.append(jnp.swapaxes(x, 0, 1)[:, None])
            x = jnp.concatenate(groups, axis=1).reshape(step * sh.tile, ch)
            rows = slice(q * sh.tile, (q + step) * sh.tile)
            hidden[rows, :] = x.astype(hidden.dtype)
            act[rows, :] = activate(x, gain_ref[...])
        pack(act, packed, sh)
        if fetch:
            copy.wait()

    got = pl.pallas_call(
        kernel,
        grid_spec=pltpu.PrefetchScalarGridSpec(
            num_scalar_prefetch=1,
            grid=(1,),
            in_specs=[pl.BlockSpec(block, row), pl.BlockSpec(block, row), full(gain)]
            + ([pl.BlockSpec(memory_space=pltpu.HBM)] if fetch else []),
            out_specs=[full(o) for o in outs],
            scratch_shapes=[pltpu.VMEM((sh.size, ch), jnp.float32), pltpu.SemaphoreType.DMA(())],
        ),
        out_shape=outs,
        name=f"first{u}",
        compiler_params=pltpu.CompilerParams(vmem_limit_bytes=40 << 20),
    )(core, mine, theirs, gain, *([kernels] if fetch else []))
    return got


def last_call(core, keeps, takens, video, sh):
    height = video.shape[1]
    count = len(keeps)
    full = lambda x: pl.BlockSpec(x.shape, lambda i, c: (0,) * x.ndim)

    def kernel(core_ref, *refs):
        out, sems = refs[2 * count], refs[2 * count + 1]
        c = core_ref[0] & 1
        copies = []
        for j in range(count):
            for part, upper in ((0, c == 0), (count, c != 0)):
                row = jnp.where(upper, j, height - 1 - j)
                copies.append(pltpu.make_async_copy(refs[part + j], out.at[:, row], sems.at[len(copies)]))
                copies[-1].start()
        for copy in copies:
            copy.wait()

    return pl.pallas_call(
        kernel,
        grid_spec=pltpu.PrefetchScalarGridSpec(
            num_scalar_prefetch=1,
            grid=(1,),
            in_specs=[full(k) for k in keeps + takens],
            out_specs=pl.BlockSpec(memory_space=pltpu.HBM),
            scratch_shapes=[pltpu.SemaphoreType.DMA((2 * count,))],
        ),
        out_shape=jax.ShapeDtypeStruct(video.shape, video.dtype),
        name="last",
        compiler_params=pltpu.CompilerParams(vmem_limit_bytes=4 << 20),
    )(core, *keeps, *takens)


def body(video, gains, kernels, count, times):
    f, height, width, ch = video.shape
    half = height // 2
    sh = Shape(width, 2 * f, ch)
    device = lambda r, t: r * times + t
    core = lax.axis_index("tm") % 2
    index = lax.axis_index("rows")
    inside = jnp.where(core == 0, index > 0, index < count - 1)
    scalar = (core.astype(jnp.int32) + 2 * inside.astype(jnp.int32))[None]
    chip = [(device(r, t), device(r, t ^ 1)) for r in range(count) for t in range(times)]
    outer = [(device(r, t), device(r + 1, t - 1)) for r in range(count - 1) for t in range(1, times, 2)]
    outer += [(b, a) for a, b in outer]
    later = [(device(r, t), device(r, t + 2)) for r in range(count) for t in range(times - 2)]
    before = (lambda rows: [lax.ppermute(row, AXES, later) for row in rows]) if times > 2 else (lambda rows: None)

    give = lax.dynamic_slice_in_dim(video, (1 - core) * half, half, axis=1)
    theirs = lax.ppermute(give, AXES, chip)
    mine = lax.dynamic_slice_in_dim(video, core * half, half, axis=1)
    gain = gains[0][None, :]
    h0, p0 = first_call(0, scalar, mine, theirs, gain, None, sh)
    h1, p1 = first_call(1, scalar, mine, theirs, gain, None, sh)
    weights = None
    hidden, packed = [h0, h1], [p0, p1]
    for layer in range(0, kernels.shape[0], 2):
        call = lambda kind, step, rows, weights, residual, partial: conv_call(
            kind, layer + step, scalar, rows, before(rows), weights, kernels, gains, residual, partial, sh
        )
        far = [lax.ppermute(row, AXES, outer) for row in packed]
        near = lax.ppermute(packed[1], AXES, chip)
        a = call("local", 0, packed + [near], weights, None, None)
        weights = a.get("w", weights)
        near = lax.ppermute(a["packed"], AXES, chip)
        b = call("outer", 0, far[:1], weights, None, [a["rest"], a["edge"]])
        got = call("local", 1, [b["packed"], a["packed"], near], a["weights"], hidden[1], None)
        c = call("edge", 0, far[1:], weights, None, [b["edge"]])
        done = call("outer", 1, [c["packed"]], a["weights"], hidden[0], [got["rest"]])
        if "packed" in got:
            hidden, packed = [done["hidden"], got["hidden"]], [done["packed"], got["packed"]]
            weights = got["weights"]

    takens = [lax.ppermute(part["give"], AXES, chip) for part in (done, got)]
    return last_call(scalar, [done["keep"], got["keep"]], takens, video, sh)


def solution(mesh):
    inner = functools.partial(body, count=mesh.shape["rows"], times=mesh.shape["tm"])
    specs = P("tm", "rows", None, None)
    return jax.shard_map(inner, mesh=mesh, in_specs=(specs, P(), P()), out_specs=specs, check_vma=False)
```

```python
import jax
import jax.numpy as jnp
from jax import lax
from jax.experimental import pallas as pl
from jax.experimental.pallas import tpu as pltpu
from jax.sharding import PartitionSpec as P


AXES = ("rows", "tm")
EPS = 1e-06
LANES = 128


def activate(x, gain):
    scale = lax.rsqrt(jnp.sum(x * x, axis=-1, keepdims=True) / x.shape[-1] + EPS)
    y = x * scale * (0.5 * gain)
    return y + y * jnp.tanh(y)


class Shape:
    def __init__(self, width, frames, channels):
        self.width, self.frames, self.channels = width, frames, channels
        self.tile = 2 * frames
        self.size = width * frames
        self.rest = channels - LANES
        self.payload = self.size + self.size // 2
        self.chunk = next(m for m in (192, 128, 64, 32, 16) if self.size % m == 0)


def unpack(ref, start, m, sh):
    half = sh.size // 2
    a = ref[start : start + m, :]
    low = start < half
    b = ref[sh.size + start - (0 if low else half) : sh.size + start - (0 if low else half) + m, :]
    b = b[:, : sh.rest] if low else b[:, sh.rest :]
    return a.astype(jnp.float32), b.astype(jnp.float32)


def build(ref, prev, s_ref, c_ref, sh):
    m = sh.tile * 8
    f, tile, n = sh.frames, sh.tile, sh.size
    edges = []
    for start in range(0, n, m):
        parts = []
        for j, x in enumerate(unpack(ref, start, m, sh)):
            x3 = x.reshape(m // f, f, x.shape[-1])
            t = lax.broadcasted_iota(jnp.int32, x3.shape, 1)
            if prev is None:
                p3 = None
            else:
                p3 = unpack(prev, start, m, sh)[j].reshape(x3.shape)
            shifted = [x]
            for step in (1, 2):
                past = jnp.zeros_like(x3) if p3 is None else pltpu.roll(p3, step, 1)
                shifted.append(jnp.where(t >= step, pltpu.roll(x3, step, 1), past).reshape(x.shape))
            parts.append(shifted)
        (a2, a1, a0), (b2, b1, b0) = parts
        whole = jnp.concatenate([a0, a1, a2, jnp.concatenate([b0, b1], axis=1)], axis=1)
        o = tile + start
        s_ref[o : o + m, :] = whole.astype(s_ref.dtype)
        b2h = b2.astype(c_ref.dtype)
        c_ref[o + tile : o + tile + m, : sh.rest] = b2h
        c_ref[o : o + m, sh.rest : 2 * sh.rest] = b2h
        c_ref[o - tile : o - tile + m, 2 * sh.rest :] = b2h
        if start == 0:
            edges.append((whole[f : 2 * f], b2[f : 2 * f]))
        if start + m == n:
            edges.append((whole[m - 2 * f : m - f], b2[m - 2 * f : m - f]))
    (first_s, first_b), (last_s, last_b) = edges
    pad = lambda v: jnp.zeros_like(v)
    s_ref[0:tile, :] = jnp.concatenate([pad(last_s), last_s], axis=0).astype(s_ref.dtype)
    s_ref[tile + n : 2 * tile + n, :] = jnp.concatenate([first_s, pad(first_s)], axis=0).astype(s_ref.dtype)
    c_ref[tile : 2 * tile, : sh.rest] = jnp.concatenate([pad(last_b), last_b], axis=0).astype(c_ref.dtype)
    c_ref[n : n + tile, 2 * sh.rest :] = jnp.concatenate([first_b, pad(first_b)], axis=0).astype(c_ref.dtype)


def taps(s_ref, c_ref, w, base, sh):
    m, total = sh.chunk, None
    for dq in range(3):
        lhs = s_ref[base + sh.tile * dq : base + sh.tile * dq + m, :]
        k = [w(dt, dq) for dt in range(3)]
        rhs = jnp.concatenate([v[:LANES] for v in k] + [v[LANES:] for v in k[:2]], axis=0)
        part = jnp.dot(lhs, rhs, preferred_element_type=jnp.float32)
        total = part if total is None else total + part
    lhs = c_ref[base + sh.tile : base + sh.tile + m, :]
    rhs = jnp.concatenate([w(2, dq)[LANES:] for dq in range(3)], axis=0)
    return total + jnp.dot(lhs, rhs, preferred_element_type=jnp.float32)


def finish(acc, base, refs, sh, second, last, inside=None):
    m = sh.chunk
    here = slice(base, base + m)
    if second:
        acc = (acc + refs["residual"][here, :].astype(jnp.float32)).astype(jnp.bfloat16)
        if last:
            refs["act"][here, :] = acc.astype(jnp.float32)
            return
        refs["hidden"][here, :] = acc
        acc = acc.astype(jnp.float32)
    value = activate(acc, refs["gain"][...])
    refs["act"][here, :] = value if inside is None else value * inside


def pack(act_ref, out_ref, sh):
    n, half = sh.size, sh.size // 2
    out_ref[0:n, :] = act_ref[:, :LANES].astype(out_ref.dtype)
    out_ref[n:, :] = jnp.concatenate([act_ref[:half, LANES:], act_ref[half:, LANES:]], axis=1).astype(out_ref.dtype)


def unpack_row(act_ref, keep_ref, give_ref, core, sh):
    f, w, ch = sh.frames, sh.width // 2, sh.channels
    step = 16
    for q in range(0, w, step):
        x = act_ref[q * sh.tile : (q + step) * sh.tile, :].reshape(step, 2, f, ch)
        for g in range(2):
            y = jnp.swapaxes(x[:, g], 0, 1)
            low, high = y[: f // 2], y[f // 2 :]
            here = slice(g * w + q, g * w + q + step)
            keep_ref[:, here, :] = jnp.where(core == 0, low, high).astype(keep_ref.dtype)
            give_ref[:, here, :] = jnp.where(core == 0, high, low).astype(give_ref.dtype)


def scratch(rows, sh):
    return [pltpu.VMEM((sh.size + 2 * sh.tile, 4 * LANES), jnp.bfloat16) for _ in range(rows)] + [
        pltpu.VMEM((sh.size + 2 * sh.tile, 3 * sh.rest), jnp.bfloat16) for _ in range(rows)
    ]


def conv_call(kind, layer, core, rows, prevs, weights, kernels, gains, residual, partial, sh):
    second, last = layer % 2 == 1, layer == kernels.shape[0] - 1
    local, edge = kind == "local", kind == "edge"
    ahead = not second and not edge
    fetch = local and not last
    n, ch = sh.size, sh.channels
    full = lambda x: pl.BlockSpec(x.shape, lambda i, c: (0,) * x.ndim)
    ins, specs, names = [], [], []

    def add(name, value, spec=None):
        ins.append(value)
        specs.append(full(value) if spec is None else spec)
        names.append(name)

    for j, row in enumerate(rows):
        add(f"row{j}", row)
    if prevs is not None:
        for j, row in enumerate(prevs):
            add(f"prev{j}", row)
    add("w", weights)
    if not local:
        add("partial", partial[0])
        if ahead:
            add("beyond", partial[1])
    if not last:
        add("gain", gains[layer + 1][None, :])
    if second:
        add("residual", residual)
    if fetch:
        add("kernels", kernels, pl.BlockSpec(memory_space=pltpu.HBM))
    outs, out_names = [], []

    def give(name, shape, dtype=jnp.bfloat16):
        outs.append(jax.ShapeDtypeStruct(shape, dtype))
        out_names.append(name)

    if local:
        give("rest", (n, ch), jnp.float32)
    if ahead:
        give("edge", (n, ch), jnp.float32)
    if last:
        give("keep", (sh.frames // 2, sh.width, ch))
        give("give", (sh.frames // 2, sh.width, ch))
    else:
        if second:
            give("hidden", (n, ch))
        give("packed", (sh.payload, LANES))
    if fetch:
        give("weights", kernels.shape[1:])
    scratches = scratch(len(rows), sh) + [pltpu.VMEM((n, ch), jnp.float32), pltpu.SemaphoreType.DMA(())]

    def kernel(core_ref, *refs):
        named = dict(zip(names + out_names, refs))
        s = refs[len(names) + len(out_names) :]
        k = len(rows)
        if fetch:
            copy = pltpu.make_async_copy(named["kernels"].at[layer + 1], named["weights"], s[2 * k + 1])
            copy.start()
        for j in range(k):
            build(named[f"row{j}"], named.get(f"prev{j}"), s[j], s[k + j], sh)
        named["act"] = s[2 * k]
        c = core_ref[0] & 1

        def weight(dr):
            index = jnp.where(c == 0, dr, 2 - dr)
            return lambda dt, dq: named["w"][dt, index, dq]

        for base in range(0, n, sh.chunk):
            here = slice(base, base + sh.chunk)
            tap = lambda row, dr: taps(s[row], s[k + row], weight(dr), base, sh)
            if local:
                named["act"][here, :] = tap(0, 0) + tap(1, 1) + tap(2, 2)
                named["rest"][here, :] = tap(0, 1) + tap(1, 2)
                if ahead:
                    named["edge"][here, :] = tap(0, 2)
            else:
                inside = (core_ref[0] >> 1).astype(jnp.float32) if edge else None
                finish(named["partial"][here, :] + tap(0, 0), base, named, sh, second, last, inside)
                if ahead:
                    named["edge"][here, :] = named["beyond"][here, :] + tap(0, 1)
        for base in range(0, n if local else 0, sh.chunk):
            finish(named["act"][base : base + sh.chunk, :], base, named, sh, second, last)
        if last:
            unpack_row(named["act"], named["keep"], named["give"], c, sh)
        else:
            pack(named["act"], named["packed"], sh)
        if fetch:
            copy.wait()

    flops = 2 * n * 9 * ch * ch * ((5 if local else 1) + ahead)
    call = pl.pallas_call(
        kernel,
        grid_spec=pltpu.PrefetchScalarGridSpec(
            num_scalar_prefetch=1,
            grid=(1,),
            in_specs=specs,
            out_specs=[full(o) for o in outs],
            scratch_shapes=scratches,
        ),
        out_shape=outs,
        cost_estimate=pl.CostEstimate(flops=flops, transcendentals=0, bytes_accessed=4 << 20),
        compiler_params=pltpu.CompilerParams(vmem_limit_bytes=40 << 20),
    )
    return dict(zip(out_names, call(core, *ins)))


def first_call(core, mine, theirs, gain, kernels, sh):
    _, half, width, ch = mine.shape
    full = lambda x: pl.BlockSpec(x.shape, lambda i, c: (0,) * x.ndim)
    outs = [jax.ShapeDtypeStruct((sh.size, ch), jnp.bfloat16) for _ in range(half)]
    outs += [jax.ShapeDtypeStruct((sh.payload, LANES), jnp.bfloat16) for _ in range(half)]
    outs.append(jax.ShapeDtypeStruct(kernels.shape[1:], kernels.dtype))

    def kernel(core_ref, own, other, gain_ref, source, *refs):
        act, sem = refs[2 * half + 1 :]
        copy = pltpu.make_async_copy(source.at[0], refs[2 * half], sem)
        copy.start()
        c, w, step = core_ref[0] & 1, width // 2, 16
        for u in range(half):
            row = jnp.where(c == 0, u, half - 1 - u)
            for q in range(0, w, step):
                groups = []
                for g in range(2):
                    here = slice(g * w + q, g * w + q + step)
                    a, b = own[:, row, here, :].astype(jnp.float32), other[:, row, here, :].astype(jnp.float32)
                    x = jnp.concatenate([jnp.where(c == 0, a, b), jnp.where(c == 0, b, a)], axis=0)
                    groups.append(jnp.swapaxes(x, 0, 1)[:, None])
                x = jnp.concatenate(groups, axis=1).reshape(step * sh.tile, ch)
                rows = slice(q * sh.tile, (q + step) * sh.tile)
                refs[u][rows, :] = x.astype(refs[u].dtype)
                act[rows, :] = activate(x, gain_ref[...])
            pack(act, refs[half + u], sh)
        copy.wait()

    got = pl.pallas_call(
        kernel,
        grid_spec=pltpu.PrefetchScalarGridSpec(
            num_scalar_prefetch=1,
            grid=(1,),
            in_specs=[full(mine), full(theirs), full(gain), pl.BlockSpec(memory_space=pltpu.HBM)],
            out_specs=[full(o) for o in outs],
            scratch_shapes=[pltpu.VMEM((sh.size, ch), jnp.float32), pltpu.SemaphoreType.DMA(())],
        ),
        out_shape=outs,
        name="first",
        compiler_params=pltpu.CompilerParams(vmem_limit_bytes=40 << 20),
    )(core, mine, theirs, gain, kernels)
    return list(got[:half]), list(got[half:-1]), got[-1]


def last_call(core, keeps, takens, video):
    height = video.shape[1]
    count = len(keeps)
    full = lambda x: pl.BlockSpec(x.shape, lambda i, c: (0,) * x.ndim)

    def kernel(core_ref, *refs):
        out, sems = refs[2 * count], refs[2 * count + 1]
        c = core_ref[0] & 1
        copies = []
        for j in range(count):
            for part, upper in ((0, c == 0), (count, c != 0)):
                row = jnp.where(upper, j, height - 1 - j)
                copies.append(pltpu.make_async_copy(refs[part + j], out.at[:, row], sems.at[len(copies)]))
                copies[-1].start()
        for copy in copies:
            copy.wait()

    return pl.pallas_call(
        kernel,
        grid_spec=pltpu.PrefetchScalarGridSpec(
            num_scalar_prefetch=1,
            grid=(1,),
            in_specs=[full(k) for k in keeps + takens],
            out_specs=pl.BlockSpec(memory_space=pltpu.HBM),
            scratch_shapes=[pltpu.SemaphoreType.DMA((2 * count,))],
        ),
        out_shape=jax.ShapeDtypeStruct(video.shape, video.dtype),
        name="last",
        compiler_params=pltpu.CompilerParams(vmem_limit_bytes=4 << 20),
    )(core, *keeps, *takens)


def body(video, gains, kernels, count, times):
    f, height, width, ch = video.shape
    half = height // 2
    sh = Shape(width, 2 * f, ch)
    device = lambda r, t: r * times + t
    core = lax.axis_index("tm") % 2
    index = lax.axis_index("rows")
    inside = jnp.where(core == 0, index > 0, index < count - 1)
    scalar = (core.astype(jnp.int32) + 2 * inside.astype(jnp.int32))[None]
    chip = [(device(r, t), device(r, t ^ 1)) for r in range(count) for t in range(times)]
    outer = [(device(r, t), device(r + 1, t - 1)) for r in range(count - 1) for t in range(1, times, 2)]
    outer += [(b, a) for a, b in outer]
    later = [(device(r, t), device(r, t + 2)) for r in range(count) for t in range(times - 2)]
    before = (lambda rows: [lax.ppermute(row, AXES, later) for row in rows]) if times > 2 else (lambda rows: None)

    give = lax.dynamic_slice_in_dim(video, (1 - core) * half, half, axis=1)
    theirs = lax.ppermute(give, AXES, chip)
    mine = lax.dynamic_slice_in_dim(video, core * half, half, axis=1)
    gain = gains[0][None, :]
    hidden, packed, weights = first_call(scalar, mine, theirs, gain, kernels, sh)
    for layer in range(0, kernels.shape[0], 2):
        call = lambda kind, step, rows, weights, residual, partial: conv_call(
            kind, layer + step, scalar, rows, before(rows), weights, kernels, gains, residual, partial, sh
        )
        far_inner = lax.ppermute(packed[1], AXES, outer)
        far_outer = lax.ppermute(packed[0], AXES, outer)
        near = lax.ppermute(packed[1], AXES, chip)
        a = call("local", 0, packed + [near], weights, None, None)
        near = lax.ppermute(a["packed"], AXES, chip)
        b = call("outer", 0, [far_outer], weights, None, [a["rest"], a["edge"]])
        got = call("local", 1, [b["packed"], a["packed"], near], a["weights"], hidden[1], None)
        c = call("edge", 0, [far_inner], weights, None, [b["edge"]])
        done = call("outer", 1, [c["packed"]], a["weights"], hidden[0], [got["rest"]])
        if "packed" in got:
            hidden, packed = [done["hidden"], got["hidden"]], [done["packed"], got["packed"]]
            weights = got["weights"]

    taken = lax.ppermute(got["give"], AXES, chip)
    takens = [lax.ppermute(done["give"], AXES, chip), taken]
    return last_call(scalar, [done["keep"], got["keep"]], takens, video)


def solution(mesh):
    specs = P("tm", "rows", None, None)

    def inner(video, gains, kernels):
        return body(video, gains, kernels, mesh.shape["rows"], mesh.shape["tm"])

    return jax.shard_map(inner, mesh=mesh, in_specs=(specs, P(), P()), out_specs=specs, check_vma=False)
```

```python
import jax
import jax.numpy as jnp
from jax import lax
from jax.experimental import pallas as pl
from jax.experimental.pallas import tpu as pltpu
from jax.sharding import PartitionSpec as P


AXES = ("rows", "tm")
EPS = 1e-06
LANES = 128


def activate(x, gain):
    scale = lax.rsqrt(jnp.sum(x * x, axis=-1, keepdims=True) / x.shape[-1] + EPS)
    y = x * scale * (0.5 * gain)
    return y + y * jnp.tanh(y)


class Shape:
    def __init__(self, width, frames, channels):
        self.width, self.frames, self.channels = width, frames, channels
        self.tile = 2 * frames
        self.size = width * frames
        self.rest = channels - LANES
        self.payload = self.size + self.size // 2
        self.chunk = next(m for m in (192, 128, 64, 32, 16) if self.size % m == 0)


def unpack(ref, start, m, sh):
    half = sh.size // 2
    a = ref[start : start + m, :]
    low = start < half
    b = ref[sh.size + start - (0 if low else half) : sh.size + start - (0 if low else half) + m, :]
    b = b[:, : sh.rest] if low else b[:, sh.rest :]
    return a.astype(jnp.float32), b.astype(jnp.float32)


def plain(ref, start, m, sh):
    return ref[start : start + m, :LANES], ref[start : start + m, LANES:]


def build(ref, prev, s_ref, c_ref, sh, load=unpack):
    m = sh.tile * 8
    f, tile, n = sh.frames, sh.tile, sh.size
    edges = []
    for start in range(0, n, m):
        parts = []
        for j, x in enumerate(load(ref, start, m, sh)):
            x3 = x.reshape(m // f, f, x.shape[-1])
            t = lax.broadcasted_iota(jnp.int32, x3.shape, 1)
            if prev is None:
                p3 = None
            else:
                p3 = unpack(prev, start, m, sh)[j].reshape(x3.shape)
            shifted = [x]
            for step in (1, 2):
                past = jnp.zeros_like(x3) if p3 is None else pltpu.roll(p3, step, 1)
                shifted.append(jnp.where(t >= step, pltpu.roll(x3, step, 1), past).reshape(x.shape))
            parts.append(shifted)
        (a2, a1, a0), (b2, b1, b0) = parts
        whole = jnp.concatenate([a0, a1, a2, jnp.concatenate([b0, b1], axis=1)], axis=1)
        o = tile + start
        s_ref[o : o + m, :] = whole.astype(s_ref.dtype)
        b2h = b2.astype(c_ref.dtype)
        c_ref[o + tile : o + tile + m, : sh.rest] = b2h
        c_ref[o : o + m, sh.rest : 2 * sh.rest] = b2h
        c_ref[o - tile : o - tile + m, 2 * sh.rest :] = b2h
        if start == 0:
            edges.append((whole[f : 2 * f], b2[f : 2 * f]))
        if start + m == n:
            edges.append((whole[m - 2 * f : m - f], b2[m - 2 * f : m - f]))
    (first_s, first_b), (last_s, last_b) = edges
    pad = lambda v: jnp.zeros_like(v)
    s_ref[0:tile, :] = jnp.concatenate([pad(last_s), last_s], axis=0).astype(s_ref.dtype)
    s_ref[tile + n : 2 * tile + n, :] = jnp.concatenate([first_s, pad(first_s)], axis=0).astype(s_ref.dtype)
    c_ref[tile : 2 * tile, : sh.rest] = jnp.concatenate([pad(last_b), last_b], axis=0).astype(c_ref.dtype)
    c_ref[n : n + tile, 2 * sh.rest :] = jnp.concatenate([first_b, pad(first_b)], axis=0).astype(c_ref.dtype)


def taps(s_ref, c_ref, w, base, sh):
    m, total = sh.chunk, None
    for dq in range(3):
        lhs = s_ref[base + sh.tile * dq : base + sh.tile * dq + m, :]
        k = [w(dt, dq) for dt in range(3)]
        rhs = jnp.concatenate([v[:LANES] for v in k] + [v[LANES:] for v in k[:2]], axis=0)
        part = jnp.dot(lhs, rhs, preferred_element_type=jnp.float32)
        total = part if total is None else total + part
    lhs = c_ref[base + sh.tile : base + sh.tile + m, :]
    rhs = jnp.concatenate([w(2, dq)[LANES:] for dq in range(3)], axis=0)
    return total + jnp.dot(lhs, rhs, preferred_element_type=jnp.float32)


def finish(acc, base, refs, sh, second, last, inside=None):
    m = sh.chunk
    here = slice(base, base + m)
    if second:
        acc = (acc + refs["residual"][here, :].astype(jnp.float32)).astype(jnp.bfloat16)
        if last:
            refs["act"][here, :] = acc.astype(jnp.float32)
            return
        refs["hidden"][here, :] = acc
        acc = acc.astype(jnp.float32)
    value = activate(acc, refs["gain"][...])
    refs["act"][here, :] = value if inside is None else value * inside


def pack(act_ref, out_ref, sh):
    n, half = sh.size, sh.size // 2
    out_ref[0:n, :] = act_ref[:, :LANES].astype(out_ref.dtype)
    out_ref[n:, :] = jnp.concatenate([act_ref[:half, LANES:], act_ref[half:, LANES:]], axis=1).astype(out_ref.dtype)


def unpack_row(act_ref, keep_ref, give_ref, core, sh):
    f, w, ch = sh.frames, sh.width // 2, sh.channels
    step = 16
    for q in range(0, w, step):
        x = act_ref[q * sh.tile : (q + step) * sh.tile, :].reshape(step, 2, f, ch)
        for g in range(2):
            y = jnp.swapaxes(x[:, g], 0, 1)
            low, high = y[: f // 2], y[f // 2 :]
            here = slice(g * w + q, g * w + q + step)
            keep_ref[:, here, :] = jnp.where(core == 0, low, high).astype(keep_ref.dtype)
            give_ref[:, here, :] = jnp.where(core == 0, high, low).astype(give_ref.dtype)


def scratch(rows, sh):
    return [pltpu.VMEM((sh.size + 2 * sh.tile, 4 * LANES), jnp.bfloat16) for _ in range(rows)] + [
        pltpu.VMEM((sh.size + 2 * sh.tile, 3 * sh.rest), jnp.bfloat16) for _ in range(rows)
    ]


def conv_call(kind, layer, core, rows, prevs, weights, kernels, gains, residual, partial, sh):
    second, last = layer % 2 == 1, layer == kernels.shape[0] - 1
    local, edge = kind == "local", kind == "edge"
    ahead = not second and not edge
    fetch = local and not last
    n, ch = sh.size, sh.channels
    full = lambda x: pl.BlockSpec(x.shape, lambda i, c: (0,) * x.ndim)
    ins, specs, names = [], [], []

    def add(name, value, spec=None):
        ins.append(value)
        specs.append(full(value) if spec is None else spec)
        names.append(name)

    for j, row in enumerate(rows):
        add(f"row{j}", row)
    if prevs is not None:
        for j, row in enumerate(prevs):
            add(f"prev{j}", row)
    add("w", weights)
    if not local:
        add("partial", partial[0])
        if ahead:
            add("beyond", partial[1])
    if not last:
        add("gain", gains[layer + 1][None, :])
    if second:
        add("residual", residual)
    if fetch:
        add("kernels", kernels, pl.BlockSpec(memory_space=pltpu.HBM))
    outs, out_names = [], []

    def give(name, shape, dtype=jnp.bfloat16):
        outs.append(jax.ShapeDtypeStruct(shape, dtype))
        out_names.append(name)

    if local:
        give("rest", (n, ch), jnp.float32)
    if ahead:
        give("edge", (n, ch), jnp.float32)
    if last:
        give("keep", (sh.frames // 2, sh.width, ch))
        give("give", (sh.frames // 2, sh.width, ch))
    else:
        if second:
            give("hidden", (n, ch))
        give("packed", (sh.payload, LANES))
    if fetch:
        give("weights", kernels.shape[1:])
    scratches = scratch(len(rows), sh) + [pltpu.VMEM((n, ch), jnp.float32), pltpu.SemaphoreType.DMA(())]

    def kernel(core_ref, *refs):
        named = dict(zip(names + out_names, refs))
        s = refs[len(names) + len(out_names) :]
        k = len(rows)
        if fetch:
            copy = pltpu.make_async_copy(named["kernels"].at[layer + 1], named["weights"], s[2 * k + 1])
            copy.start()
        for j in range(k):
            build(named[f"row{j}"], named.get(f"prev{j}"), s[j], s[k + j], sh)
        named["act"] = s[2 * k]
        c = core_ref[0] & 1

        def weight(dr):
            index = jnp.where(c == 0, dr, 2 - dr)
            return lambda dt, dq: named["w"][dt, index, dq]

        for base in range(0, n, sh.chunk):
            here = slice(base, base + sh.chunk)
            tap = lambda row, dr: taps(s[row], s[k + row], weight(dr), base, sh)
            if local:
                named["act"][here, :] = tap(0, 0) + tap(1, 1) + tap(2, 2)
                named["rest"][here, :] = tap(0, 1) + tap(1, 2)
                if ahead:
                    named["edge"][here, :] = tap(0, 2)
            else:
                inside = (core_ref[0] >> 1).astype(jnp.float32) if edge else None
                finish(named["partial"][here, :] + tap(0, 0), base, named, sh, second, last, inside)
                if ahead:
                    named["edge"][here, :] = named["beyond"][here, :] + tap(0, 1)
        for base in range(0, n if local else 0, sh.chunk):
            finish(named["act"][base : base + sh.chunk, :], base, named, sh, second, last)
        if last:
            unpack_row(named["act"], named["keep"], named["give"], c, sh)
        else:
            pack(named["act"], named["packed"], sh)
        if fetch:
            copy.wait()

    flops = 2 * n * 9 * ch * ch * ((5 if local else 1) + ahead)
    call = pl.pallas_call(
        kernel,
        grid_spec=pltpu.PrefetchScalarGridSpec(
            num_scalar_prefetch=1,
            grid=(1,),
            in_specs=specs,
            out_specs=[full(o) for o in outs],
            scratch_shapes=scratches,
        ),
        out_shape=outs,
        cost_estimate=pl.CostEstimate(flops=flops, transcendentals=0, bytes_accessed=4 << 20),
        compiler_params=pltpu.CompilerParams(vmem_limit_bytes=40 << 20),
    )
    return dict(zip(out_names, call(core, *ins)))


def beyond_call(layer, core, row, weights, gains, residual, partial, count, sh):
    last = layer == count - 1
    n, ch = sh.size, sh.channels
    full = lambda x: pl.BlockSpec(x.shape, lambda i, c: (0,) * x.ndim)
    ins = [row, *weights, *partial, residual, gains[layer][None, :]] + ([] if last else [gains[layer + 1][None, :]])
    if last:
        names = ["keep", "give"]
        outs = [jax.ShapeDtypeStruct((sh.frames // 2, sh.width, ch), jnp.bfloat16) for _ in names]
    else:
        names = ["hidden", "packed"]
        outs = [jax.ShapeDtypeStruct(x, jnp.bfloat16) for x in ((n, ch), (sh.payload, LANES))]

    def kernel(core_ref, row_ref, w0, w1, part0, part1, residual_ref, *refs):
        gain_refs, refs = refs[: len(ins) - 6], refs[len(ins) - 6 :]
        s0, s1, c0, c1, act0, act1 = refs[2:]
        c = core_ref[0] & 1
        inside = (core_ref[0] >> 1).astype(jnp.float32)
        index = jnp.where(c == 0, 0, 2)
        build(row_ref, None, s0, c0, sh)
        edge = {"act": act0, "gain": gain_refs[0]}
        named = dict(zip(names, refs)) | {"act": act1, "gain": gain_refs[-1], "residual": residual_ref}
        for base in range(0, n, sh.chunk):
            acc = part0[base : base + sh.chunk, :] + taps(s0, c0, lambda dt, dq: w0[dt, index, dq], base, sh)
            finish(acc, base, edge, sh, False, False, inside)
        build(act0, None, s1, c1, sh, plain)
        for base in range(0, n, sh.chunk):
            acc = part1[base : base + sh.chunk, :] + taps(s1, c1, lambda dt, dq: w1[dt, index, dq], base, sh)
            finish(acc, base, named, sh, True, last)
        if last:
            unpack_row(act1, named["keep"], named["give"], c, sh)
        else:
            pack(act1, named["packed"], sh)

    call = pl.pallas_call(
        kernel,
        grid_spec=pltpu.PrefetchScalarGridSpec(
            num_scalar_prefetch=1,
            grid=(1,),
            in_specs=[full(x) for x in ins],
            out_specs=[full(o) for o in outs],
            scratch_shapes=scratch(2, sh) + [pltpu.VMEM((n, ch), jnp.float32) for _ in range(2)],
        ),
        out_shape=outs,
        cost_estimate=pl.CostEstimate(flops=36 * n * ch * ch, transcendentals=0, bytes_accessed=4 << 20),
        compiler_params=pltpu.CompilerParams(vmem_limit_bytes=40 << 20),
    )
    return dict(zip(names, call(core, *ins)))


def first_call(core, mine, theirs, gain, kernels, sh):
    _, half, width, ch = mine.shape
    full = lambda x: pl.BlockSpec(x.shape, lambda i, c: (0,) * x.ndim)
    outs = [jax.ShapeDtypeStruct((sh.size, ch), jnp.bfloat16) for _ in range(half)]
    outs += [jax.ShapeDtypeStruct((sh.payload, LANES), jnp.bfloat16) for _ in range(half)]
    outs.append(jax.ShapeDtypeStruct(kernels.shape[1:], kernels.dtype))

    def kernel(core_ref, own, other, gain_ref, source, *refs):
        act, sem = refs[2 * half + 1 :]
        copy = pltpu.make_async_copy(source.at[0], refs[2 * half], sem)
        copy.start()
        c, w, step = core_ref[0] & 1, width // 2, 16
        for u in range(half):
            row = jnp.where(c == 0, u, half - 1 - u)
            for q in range(0, w, step):
                groups = []
                for g in range(2):
                    here = slice(g * w + q, g * w + q + step)
                    a, b = own[:, row, here, :].astype(jnp.float32), other[:, row, here, :].astype(jnp.float32)
                    x = jnp.concatenate([jnp.where(c == 0, a, b), jnp.where(c == 0, b, a)], axis=0)
                    groups.append(jnp.swapaxes(x, 0, 1)[:, None])
                x = jnp.concatenate(groups, axis=1).reshape(step * sh.tile, ch)
                rows = slice(q * sh.tile, (q + step) * sh.tile)
                refs[u][rows, :] = x.astype(refs[u].dtype)
                act[rows, :] = activate(x, gain_ref[...])
            pack(act, refs[half + u], sh)
        copy.wait()

    got = pl.pallas_call(
        kernel,
        grid_spec=pltpu.PrefetchScalarGridSpec(
            num_scalar_prefetch=1,
            grid=(1,),
            in_specs=[full(mine), full(theirs), full(gain), pl.BlockSpec(memory_space=pltpu.HBM)],
            out_specs=[full(o) for o in outs],
            scratch_shapes=[pltpu.VMEM((sh.size, ch), jnp.float32), pltpu.SemaphoreType.DMA(())],
        ),
        out_shape=outs,
        name="first",
        compiler_params=pltpu.CompilerParams(vmem_limit_bytes=40 << 20),
    )(core, mine, theirs, gain, kernels)
    return list(got[:half]), list(got[half:-1]), got[-1]


def last_call(core, parts, into, shape, dtype):
    rows = [part[0] for part in parts]
    height = shape[1]
    full = lambda x: pl.BlockSpec(x.shape, lambda i, c: (0,) * x.ndim)
    hbm = pl.BlockSpec(memory_space=pltpu.HBM)

    def kernel(core_ref, *refs):
        out, sems = refs[-2:]
        c = core_ref[0] & 1
        copies = []
        for j, (_, place, partner) in enumerate(parts):
            row = jnp.where(c == int(partner), place, height - 1 - place)
            copies.append(pltpu.make_async_copy(refs[j], out.at[:, row], sems.at[j]))
            copies[-1].start()
        for copy in copies:
            copy.wait()

    return pl.pallas_call(
        kernel,
        grid_spec=pltpu.PrefetchScalarGridSpec(
            num_scalar_prefetch=1,
            grid=(1,),
            in_specs=[full(row) for row in rows] + ([] if into is None else [hbm]),
            out_specs=hbm,
            scratch_shapes=[pltpu.SemaphoreType.DMA((len(rows),))],
        ),
        out_shape=jax.ShapeDtypeStruct(shape, dtype),
        input_output_aliases={} if into is None else {1 + len(rows): 0},
        name="last",
        compiler_params=pltpu.CompilerParams(vmem_limit_bytes=4 << 20),
    )(core, *rows, *([] if into is None else [into]))


def body(video, gains, kernels, count, times):
    f, height, width, ch = video.shape
    half = height // 2
    sh = Shape(width, 2 * f, ch)
    device = lambda r, t: r * times + t
    core = lax.axis_index("tm") % 2
    index = lax.axis_index("rows")
    inside = jnp.where(core == 0, index > 0, index < count - 1)
    scalar = (core.astype(jnp.int32) + 2 * inside.astype(jnp.int32))[None]
    chip = [(device(r, t), device(r, t ^ 1)) for r in range(count) for t in range(times)]
    outer = [(device(r, t), device(r + 1, t - 1)) for r in range(count - 1) for t in range(1, times, 2)]
    outer += [(b, a) for a, b in outer]
    later = [(device(r, t), device(r, t + 2)) for r in range(count) for t in range(times - 2)]
    before = (lambda rows: [lax.ppermute(row, AXES, later) for row in rows]) if times > 2 else (lambda rows: None)

    give = lax.dynamic_slice_in_dim(video, (1 - core) * half, half, axis=1)
    theirs = lax.ppermute(give, AXES, chip)
    mine = lax.dynamic_slice_in_dim(video, core * half, half, axis=1)
    gain = gains[0][None, :]
    hidden, packed, weights = first_call(scalar, mine, theirs, gain, kernels, sh)
    for layer in range(0, kernels.shape[0], 2):
        call = lambda kind, step, rows, weights, residual, partial: conv_call(
            kind, layer + step, scalar, rows, before(rows), weights, kernels, gains, residual, partial, sh
        )
        far_inner = lax.ppermute(packed[1], AXES, outer)
        far_outer = lax.ppermute(packed[0], AXES, outer)
        near = lax.ppermute(packed[1], AXES, chip)
        a = call("local", 0, packed + [near], weights, None, None)
        near = lax.ppermute(a["packed"], AXES, chip)
        b = call("outer", 0, [far_outer], weights, None, [a["rest"], a["edge"]])
        got = call("local", 1, [b["packed"], a["packed"], near], a["weights"], hidden[1], None)
        if times > 2:
            c = call("edge", 0, [far_inner], weights, None, [b["edge"]])
            done = call("outer", 1, [c["packed"]], a["weights"], hidden[0], [got["rest"]])
        else:
            both, parts = [weights, a["weights"]], [b["edge"], got["rest"]]
            done = beyond_call(layer + 1, scalar, far_inner, both, gains, hidden[0], parts, kernels.shape[0], sh)
        if "packed" in got:
            hidden, packed = [done["hidden"], got["hidden"]], [done["packed"], got["packed"]]
            weights = got["weights"]

    taken = lax.ppermute(got["give"], AXES, chip)
    late = lax.ppermute(done["give"], AXES, chip)
    early = [(done["keep"], 0, False), (got["keep"], 1, False), (taken, 1, True)]
    result = last_call(scalar, early, None, video.shape, video.dtype)
    return last_call(scalar, [(late, 0, True)], result, video.shape, video.dtype)


def solution(mesh):
    specs = P("tm", "rows", None, None)

    def inner(video, gains, kernels):
        return body(video, gains, kernels, mesh.shape["rows"], mesh.shape["tm"])

    return jax.shard_map(inner, mesh=mesh, in_specs=(specs, P(), P()), out_specs=specs, check_vma=False)
```
